256 devices in a mesh: blk: 32 (over y_hi, z, core), dp: 8 (over x, y_lo).
Axes of the slice: x: 4, y: 4 (y_hi: 2, y_lo: 2; y = y_hi * 2 + y_lo), z: 8, core: 2. Of those that a mesh axis runs over, the one named last changes fastest.
Arguments:
- query_feats: bfloat16 [8, 12288, 1024], P('dp', 'blk'), may hold values from -12 to 12
- item_feats: bfloat16 [8, 12288, 1024], P('dp', 'blk'), may hold values from -12 to 12
- item_ids: int32 [8, 12288], P('dp', 'blk'), may hold values from 0 to 1048575
- bucket_ids: int32 [8, 12288], P('dp', 'blk'), may hold values from 0 to 255
- bucket_logq: float32 [256], replicated, may hold values from -7 to -5.5
- query_tower: bfloat16 [1024, 256], replicated, may hold values from -0.1875 to 0.1875
- item_tower: bfloat16 [1024, 256], replicated, may hold values from -0.1875 to 0.1875
Outputs:
- grad_query_tower: float32 [1024, 256], replicated
- grad_item_tower: float32 [1024, 256], replicated
- loss: float32 [], replicated
The draws below stay inside these ranges and needn't reach their ends.
All inputs are finite; a program needn't handle non-finite values.
Results may differ from the reference program's by a relative error of at most 0.0041.
Values may be sent and summed in bfloat16 or wider, within the bound.
No kernel may reach another device: no remote copies, remote signals or barrier semaphores. Data moves between devices by JAX's collectives and lax.ppermute only.
A program may use at most 128 MiB of HBM per device.

```python
import math
import jax
import jax.numpy as jnp
import numpy as np
from jax import lax

F = 1024
E = 256
TOK_DEV = 384
NB = 256
ID_RANGE = 1048576
GROUP = 12288
N_DP = 8


def paired_feats(key):
    base = jax.random.fold_in(key, 101)
    keys = [jax.random.fold_in(base, number) for number in range(8)]
    shape = (N_DP, GROUP, F)
    query_side = jax.random.truncated_normal(keys[0], -6.0, 6.0, shape, jnp.float32)
    item_side = jax.random.truncated_normal(keys[1], -6.0, 6.0, shape, jnp.float32)
    return (query_side, item_side)


def paired_towers(key):
    base = jax.random.fold_in(key, 202)
    first = jax.random.fold_in(base, 1)
    second = jax.random.fold_in(base, 2)
    factor = 1.0 / math.sqrt(F)
    query_weight = jax.random.truncated_normal(first, -6.0, 6.0, (F, E), jnp.float32) * factor
    item_weight = jax.random.truncated_normal(second, -6.0, 6.0, (F, E), jnp.float32) * factor
    return (query_weight, item_weight)


def draw_query_feats(key, part):
    return paired_feats(key)[0].astype(jnp.bfloat16)


def draw_item_feats(key, part):
    return paired_feats(key)[1].astype(jnp.bfloat16)


def draw_query_tower(key, part):
    return paired_towers(key)[0].astype(jnp.bfloat16)


def draw_item_tower(key, part):
    return paired_towers(key)[1].astype(jnp.bfloat16)


def plant(values, key, least, high):
    spot = [jax.random.randint(jax.random.fold_in(key, axis), (), 0, length) for axis, length in enumerate(values.shape)]
    main_axis = values.shape.index(max(values.shape))
    neighbour = spot[:main_axis] + [(spot[main_axis] + 1) % values.shape[main_axis]] + spot[main_axis + 1:]
    return values.at[tuple(spot)].set(least).at[tuple(neighbour)].set(high)


def ranked_wide(stream_key, extent, number_of, slope):
    portions = [min(1 << octave, number_of + 1 - (1 << octave)) * (1 << 20) // math.isqrt((1 << octave) ** slope) + 1 for octave in range((number_of + 1).bit_length()) if 1 << octave <= number_of]
    deviation = 1 + sum(portions) // (1 << 30)
    listing = np.cumsum(np.array([max(1, weight // deviation) for weight in portions]))
    lot = jax.random.randint(jax.random.fold_in(stream_key, 1), extent, 0, int(listing[len(portions) - 1]))
    start = jnp.left_shift(1, jnp.searchsorted(jnp.asarray(listing, jnp.int32), lot, side="right").astype(jnp.int32))
    standing = start - 1 + jax.random.randint(jax.random.fold_in(stream_key, 4), extent, 0, 1 << 30) % jnp.minimum(start, number_of + 1 - start)
    return jax.random.permutation(jax.random.fold_in(stream_key, 2), number_of)[standing].astype(jnp.int32)


def setup_inputs(seed: int = 0) -> dict:
    key_list = jax.random.split(jax.random.key(seed), 8)
    query_feats = draw_query_feats(jax.random.fold_in(key_list[7], 71), 0)
    item_feats = draw_item_feats(jax.random.fold_in(key_list[7], 71), 0)
    item_ids = plant(ranked_wide(key_list[2], (N_DP, GROUP), ID_RANGE, 2), jax.random.fold_in(key_list[2], 3), 0, ID_RANGE - 1).astype(jnp.int32)
    bucket_ids = plant(jax.random.randint(key_list[3], (N_DP, GROUP), 0, NB), jax.random.fold_in(key_list[3], 1), 0, NB - 1).astype(jnp.int32)
    bucket_logq = jnp.clip(jax.random.uniform(key_list[4], (NB,), jnp.float32, -7.0, -5.5), -7.0, -5.5)
    query_tower = draw_query_tower(jax.random.fold_in(key_list[7], 71), 0)
    item_tower = draw_item_tower(jax.random.fold_in(key_list[7], 71), 0)
    return dict(query_feats=query_feats, item_feats=item_feats, item_ids=item_ids, bucket_ids=bucket_ids, bucket_logq=bucket_logq, query_tower=query_tower, item_tower=item_tower)


EXCLUDED = -1e+30

def contract_last(left, right):
    return lax.dot_general(left, right, (((1,), (1,)), ((), ())), preferred_element_type=jnp.float32)

def contract_first(left, right):
    return lax.dot_general(left, right, (((0,), (0,)), ((), ())), preferred_element_type=jnp.float32)

def group_terms(query_input, item_input, group_ids, group_buckets, bucket_logq, query_tower, item_tower):
    scaling = 1.0 / math.sqrt(E)
    query_vecs = jnp.dot(query_input, query_tower, preferred_element_type=jnp.float32).astype(jnp.bfloat16)
    item_vecs = jnp.dot(item_input, item_tower, preferred_element_type=jnp.float32).astype(jnp.bfloat16)
    correction = bucket_logq[group_buckets]
    columns = jnp.arange(GROUP, dtype=jnp.int32)
    blocks = GROUP // TOK_DEV
    query_blocks = query_vecs.reshape(blocks, TOK_DEV, E)
    id_blocks = group_ids.reshape(blocks, TOK_DEV)
    item_blocks = item_vecs.reshape(blocks, TOK_DEV, E)

    def block_step(item_sums, inputs):
        index, block_vecs, block_ids, block_items = inputs
        offset = (index * TOK_DEV).astype(jnp.int32)
        scores = contract_last(block_vecs, item_vecs) * scaling - correction[None, :]
        rows_global = offset + jnp.arange(TOK_DEV, dtype=jnp.int32)
        duplicate = (group_ids[None, :] == block_ids[:, None]) & (columns[None, :] != rows_global[:, None])
        masked = jnp.where(duplicate, EXCLUDED, scores)
        peaks = lax.optimization_barrier(jnp.max(masked, axis=1))
        log_total = peaks + jnp.log(lax.optimization_barrier(jnp.sum(jnp.exp(masked - peaks[:, None]), axis=1)))
        softmax = jnp.exp(masked - log_total[:, None]).astype(jnp.bfloat16)
        positive = jnp.diagonal(lax.dynamic_slice_in_dim(scores, offset, TOK_DEV, 1))
        loss_local = jnp.sum(log_total - positive)
        query_grad = ((jnp.dot(softmax, item_vecs, preferred_element_type=jnp.float32) - block_items.astype(jnp.float32)) * scaling).astype(jnp.bfloat16)
        item_sums = item_sums + contract_first(softmax, block_vecs)
        return (item_sums, (query_grad, loss_local))
    initial = jnp.zeros((GROUP, E), jnp.float32)
    item_sums, (query_grads, losses) = lax.scan(block_step, initial, (jnp.arange(blocks, dtype=jnp.int32), query_blocks, id_blocks, item_blocks))
    query_grads = query_grads.reshape(GROUP, E)
    item_grad = ((item_sums - query_vecs.astype(jnp.float32)) * scaling).astype(jnp.bfloat16)
    tower_query = contract_first(query_input, query_grads)
    tower_item = contract_first(item_input, item_grad)
    return (tower_query, tower_item, jnp.sum(losses))

def reference(query_feats, item_feats, item_ids, bucket_ids, bucket_logq, query_tower, item_tower):

    def one_group(inputs):
        return group_terms(inputs[0], inputs[1], inputs[2], inputs[3], bucket_logq, query_tower, item_tower)
    tower_query, tower_item, losses = lax.map(one_group, (query_feats, item_feats, item_ids, bucket_ids))
    return (lax.optimization_barrier(jnp.sum(tower_query, axis=0)), lax.optimization_barrier(jnp.sum(tower_item, axis=0)), jnp.sum(losses) / (N_DP * GROUP))
```

```python
import functools

import jax
import jax.numpy as jnp
from jax import lax
from jax.experimental import pallas as pl
from jax.experimental.pallas import tpu as pltpu
from jax.sharding import Mesh
from jax.sharding import PartitionSpec as P

EXCLUDED = -1e30
BLK = ("yh", "z", "c")
DP = ("x", "yl")
META = 16

f32, bf16 = jnp.float32, jnp.bfloat16


def dot(a, b, ca, cb):
    return lax.dot_general(a, b, (((ca,), (cb,)), ((), ())), preferred_element_type=f32)


def shift(x, axis, by):
    n = lax.axis_size(axis)
    return lax.ppermute(x, axis, [(i, (i + by) % n) for i in range(n)])


def split3(x):
    hi = lax.reduce_precision(x, 8, 7)
    rest = x - hi
    mid = lax.reduce_precision(rest, 8, 7)
    return hi, mid, rest - mid


def join_meta(meta, at, scales):
    v = meta.astype(f32)
    left = sum(v[at + 2 * k : at + 2 * k + 1, :] * s for k, s in enumerate(scales))
    right = sum(v[at + 2 * k + 1 : at + 2 * k + 2, :128] * s for k, s in enumerate(scales))
    return jnp.concatenate([left, right], axis=1)


def ids_of(meta):
    return join_meta(meta, 0, (65536.0, 256.0, 1.0))


def corrections_of(meta):
    return join_meta(meta, 6, (1.0, 1.0, 1.0))


def down(row):
    return jnp.transpose(jnp.broadcast_to(row, (128, 128)))


def across(col):
    return jnp.transpose(col)[:1, :]


def prep_kernel(rows, b0, b1, b2, b3, q_ref, qt_ref, id_ref):
    for k, b in enumerate((b0, b1, b2, b3)):
        v = b[:rows, :].astype(f32)
        q_ref[k * rows : (k + 1) * rows, :] = (v * 0.0625).astype(bf16)
        qt_ref[:, k * rows : (k + 1) * rows] = jnp.transpose(v).astype(bf16)
        ids = ids_of(b[rows : rows + META, :])
        for j in range(rows // 128):
            id_ref[k * rows + j * 128 : k * rows + (j + 1) * 128, :] = down(ids[:, j * 128 : (j + 1) * 128])


def prep(blocks):
    rows = blocks[0].shape[0] - META
    wide = blocks[0].shape[1]
    return pl.pallas_call(
        functools.partial(prep_kernel, rows),
        out_shape=(
            jax.ShapeDtypeStruct((4 * rows, wide), bf16),
            jax.ShapeDtypeStruct((wide, 4 * rows), bf16),
            jax.ShapeDtypeStruct((4 * rows, 128), f32),
        ),
        name="prep",
    )(*blocks)


def step_kernel(first, last, nb, rows, tm, *refs):
    q_ref, id_ref = refs[:2]
    blocks = refs[2 : 2 + nb]
    at = 2 + nb
    if not first:
        m_in, l_in, ok_in, os_in = refs[at : at + 4]
        at += 4
    p_ref, m_out, l_out, ok_out, os_out, md_ref, lse_ref = refs[at : at + 7]
    pid = pl.program_id(0)
    half = pl.num_programs(0) // 2
    items = jnp.concatenate([b[:rows, :] for b in blocks], axis=0) if nb > 1 else blocks[0][:rows, :]
    col_ids = jnp.concatenate([ids_of(b[rows : rows + META, :]) for b in blocks], axis=1)
    corr = jnp.concatenate([corrections_of(b[rows : rows + META, :]) for b in blocks], axis=1)
    cols = nb * rows
    s = dot(q_ref[...], items, 1, 1) - corr
    dup = id_ref[:, :1] == col_ids
    if first:
        row = lax.broadcasted_iota(jnp.int32, (tm, cols), 0) + pid * tm
        col = lax.broadcasted_iota(jnp.int32, (tm, cols), 1)
        dup = dup & (row != col)
    s = jnp.where(dup, EXCLUDED, s)
    m = jnp.max(s, axis=1, keepdims=True)
    if not first:
        m_old = m_in[:, :1]
        m = jnp.maximum(m, m_old)
    p = jnp.exp(s - m)
    l = jnp.sum(p, axis=1, keepdims=True)
    pb = p.astype(bf16)
    p_ref[...] = pb
    o = dot(pb, items, 1, 0)
    if not first:
        a = jnp.exp(m_old - m)
        l = l + a * l_in[:, :1]
    mw = jnp.broadcast_to(m, (tm, 128))
    if last:
        lse = jnp.broadcast_to(m + jnp.log(l), (tm, 128))
    else:
        m_out[...] = mw
        l_out[...] = jnp.broadcast_to(l, (tm, 128))
    for j in range(tm // 128):
        md_ref[:, j * 128 : (j + 1) * 128] = across(mw[j * 128 : (j + 1) * 128, :])
        if last:
            lse_ref[:, j * 128 : (j + 1) * 128] = across(lse[j * 128 : (j + 1) * 128, :])

    def put(o_out, o_in):
        v = o if first else o + a * o_in[...]
        o_out[...] = v * (1.0 / l) if last else v

    @pl.when(pid < half)
    def _():
        put(ok_out, None if first else ok_in)

    @pl.when(pid >= half)
    def _():
        put(os_out, None if first else os_in)


def step(q, ids, blocks, state, last=False, tm=256):
    n, wide = q.shape
    nb, rows = len(blocks), blocks[0].shape[0] - META
    first = state is None
    grid = n // tm
    half = grid // 2
    by_row = lambda w: pl.BlockSpec((tm, w), lambda i: (i, 0))
    keep = pl.BlockSpec((tm, wide), lambda i: (jnp.minimum(i, half - 1), 0))
    send = pl.BlockSpec((tm, wide), lambda i: (jnp.maximum(i - half, 0), 0))
    dense = pl.BlockSpec((1, tm), lambda i: (0, i))
    in_specs = [by_row(wide), by_row(128)]
    in_specs += [pl.BlockSpec((rows + META, wide), lambda i: (0, 0))] * nb
    args = [q, ids, *blocks]
    if not first:
        in_specs += [by_row(128), by_row(128), keep, send]
        args += list(state)
    ml = jax.ShapeDtypeStruct((8, 128) if last else (n, 128), f32)
    ml_spec = pl.BlockSpec((8, 128), lambda i: (0, 0)) if last else by_row(128)
    p, m, l, ok, os, md, lse = pl.pallas_call(
        functools.partial(step_kernel, first, last, nb, rows, tm),
        grid=(grid,),
        in_specs=in_specs,
        out_specs=(by_row(nb * rows), ml_spec, ml_spec, keep, send, dense, dense),
        out_shape=(
            jax.ShapeDtypeStruct((n, nb * rows), bf16),
            ml,
            ml,
            jax.ShapeDtypeStruct((n // 2, wide), f32),
            jax.ShapeDtypeStruct((n // 2, wide), f32),
            jax.ShapeDtypeStruct((1, n), f32),
            jax.ShapeDtypeStruct((1, n), f32),
        ),
        cost_estimate=pl.CostEstimate(
            flops=4 * n * nb * rows * wide, bytes_accessed=n * (nb * rows * 2 + 4 * wide * 2), transcendentals=n * nb * rows
        ),
        name="scores",
    )(*args)
    return p, (m, l, ok, os), md, lse


def back_kernel(qt_ref, p_ref, md_ref, lse_ref, *outs):
    w = jnp.exp(md_ref[...] - lse_ref[...])
    qw = (qt_ref[...].astype(f32) * w).astype(bf16)
    t = dot(qw, p_ref[...], 1, 0)
    rows = t.shape[1] // len(outs)
    for k, o in enumerate(outs):
        o[...] = t[:, k * rows : (k + 1) * rows].astype(o.dtype)


def back(qt, p, md, lse, nb, dtype):
    wide, n = qt.shape
    rows = p.shape[1] // nb
    return pl.pallas_call(
        back_kernel,
        out_shape=[jax.ShapeDtypeStruct((wide, rows), dtype)] * nb,
        cost_estimate=pl.CostEstimate(flops=2 * n * nb * rows * wide, bytes_accessed=n * nb * rows * 2, transcendentals=n),
        name="back",
    )(qt, p, md, lse)


def log_add(a, b):
    top = jnp.maximum(a, b)
    return top + jnp.log(jnp.exp(a - top) + jnp.exp(b - top))


def merge_kernel(a_ref, b_ref, la_ref, lb_ref, o_ref):
    la, lb = la_ref[...], lb_ref[...]
    top = jnp.maximum(la, lb)
    ea, eb = jnp.exp(la - top), jnp.exp(lb - top)
    wa, wb = ea / (ea + eb), eb / (ea + eb)
    for j in range(la.shape[1] // 128):
        at = slice(j * 128, (j + 1) * 128)
        ca, cb = down(wa[:, at])[:, :1], down(wb[:, at])[:, :1]
        o_ref[at, :] = (a_ref[at, :].astype(f32) * ca + b_ref[at, :].astype(f32) * cb).astype(o_ref.dtype)


def merge(a, b, la, lb):
    return pl.pallas_call(merge_kernel, out_shape=jax.ShapeDtypeStruct(a.shape, f32), name="merge")(a, b, la, lb)


def on_device(query_feats, item_feats, item_ids, bucket_ids, bucket_logq, query_tower, item_tower):
    query_input, item_input = query_feats[0], item_feats[0]
    rows = query_input.shape[0]
    wide = query_tower.shape[1]
    own_ids, own_buckets = item_ids[0], bucket_ids[0]
    scaling = 1.0 / 16.0
    buckets = jnp.arange(bucket_logq.shape[0], dtype=jnp.int32)
    correction = jnp.sum(jnp.where(own_buckets[:, None] == buckets[None, :], bucket_logq[None, :], 0.0), axis=1)
    pieces = [own_ids // 65536, (own_ids // 256) % 256, own_ids % 256]
    pieces = [p.astype(f32) for p in pieces] + list(split3(correction))
    meta = jnp.stack([jnp.pad(p, (0, 512 - rows)) for p in pieces]).reshape(12, 256)
    meta = jnp.pad(meta, ((0, META - 12), (0, 0))).astype(bf16)
    item_vecs = jnp.dot(item_input, item_tower, preferred_element_type=f32).astype(bf16)
    query_vecs = jnp.dot(query_input, query_tower, preferred_element_type=f32).astype(bf16)
    item_block = jnp.concatenate([item_vecs, meta])
    query_block = jnp.concatenate([query_vecs, meta])

    near = shift(query_block, "yh", 1)
    up, dn = [item_block], [item_block]
    up.append(shift(up[-1], "z", 1))
    dn.append(shift(dn[-1], "z", -1))
    pair = jnp.concatenate([query_block, near])
    other = shift(pair, "c", 1)
    q, qt, ids = prep((query_block, near, other[: rows + META], other[rows + META :]))
    p0, state, md0, _ = step(q, ids, [item_block], None)
    ps, mds = [p0], [md0]
    for k in range(1, 4):
        if k < 3:
            up.append(shift(up[-1], "z", 1))
            dn.append(shift(dn[-1], "z", -1))
        else:
            up.append(shift(up[-1], "z", 1))
        pk, state, md, _ = step(q, ids, [up[k], dn[k]], state)
        ps.append(pk)
        mds.append(md)
    p4, (_, _, o_keep, o_send), md4, lse_part = step(q, ids, [up[4]], state, last=True)

    def swapped(row, bit):
        return jnp.concatenate([row[:, (k ^ bit) * rows : ((k ^ bit) + 1) * rows] for k in range(4)], axis=1)

    lse_c = swapped(shift(lse_part, "c", 1), 2)
    o_c = shift(o_send, "c", 1)
    lse_2 = log_add(lse_part, lse_c)
    lse_y = swapped(shift(lse_2, "yh", 1), 1)
    lse = log_add(lse_2, lse_y)

    back4 = back(qt, p4, md4, lse, 1, bf16)[0]
    ring_up = shift(back4, "z", 1)
    o_2 = merge(o_keep, o_c, lse_part[:, : 2 * rows], lse_c[:, : 2 * rows])
    o_y = shift(o_2[rows:].astype(bf16), "yh", 1)
    ring_dn = None
    for k in (3, 2, 1):
        t_dn, t_up = back(qt, ps[k], mds[k], lse, 2, f32)
        new_up = (ring_up.astype(f32) + t_up).astype(bf16)
        new_dn = t_dn if ring_dn is None else ring_dn.astype(f32) + t_dn
        ring_up = shift(new_up, "z", 1)
        ring_dn = shift(new_dn.astype(bf16), "z", -1)
    t_own = back(qt, p0, md0, lse, 1, f32)[0]
    o = merge(o_2[:rows], o_y, lse_2[:, :rows], lse_y[:, :rows])
    query_grad = ((o - item_vecs.astype(f32)) * scaling).astype(bf16)
    tower_query = dot(query_grad, query_input, 0, 0)
    loss_local = jnp.sum(lse[:, :rows]) - (
        jnp.sum(query_vecs.astype(f32) * item_vecs.astype(f32)) * scaling - jnp.sum(correction)
    )
    item_sums = t_own + ring_up.astype(f32) + ring_dn.astype(f32)
    item_grad = ((item_sums - qt[:, :rows].astype(f32)) * scaling).astype(bf16)
    tower_item = dot(item_grad, item_input, 1, 0)

    core = lax.axis_index("c")
    keep = jnp.where(core == 0, tower_query, tower_item)
    give = jnp.where(core == 0, tower_item, tower_query)
    half = keep + shift(give, "c", 1)
    chips = ("yh", "z", "x", "yl")
    n = lax.axis_size(chips)
    feats = half.shape[1]
    tr, tc = 16, 128
    tiles = half.reshape(wide // tr, tr, feats // tc, tc).transpose(0, 2, 1, 3).reshape(n, tr, tc)
    loss3 = jnp.stack(split3(loss_local + shift(loss_local, "c", 1)))
    loss_rows = jnp.broadcast_to(jnp.pad(loss3, (0, 5))[None, :, None], (n, 8, tc))
    parts = lax.all_to_all(jnp.concatenate([tiles, loss_rows], axis=1).astype(bf16), chips, 0, 0, tiled=True)
    total = jnp.sum(parts.astype(f32), axis=0)
    loss = jnp.sum(total[tr : tr + 3, 0])
    mine = total[:tr].astype(bf16)
    everything = lax.all_to_all(jnp.broadcast_to(mine[None], (n, tr, tc)), chips, 0, 0, tiled=True)
    half = everything.reshape(wide // tr, feats // tc, tr, tc).transpose(0, 2, 1, 3).reshape(wide, feats)
    rest = shift(half, "c", 1)
    grad_query = jnp.where(core == 0, half, rest).astype(f32).T
    grad_item = jnp.where(core == 0, rest, half).astype(f32).T
    count = lax.axis_size(BLK) * rows * lax.axis_size(DP)
    return (grad_query, grad_item, loss / count)


def solution(mesh):
    fine = Mesh(mesh.devices.reshape(2, 8, 2, 4, 2), ("yh", "z", "c", "x", "yl"))
    return jax.shard_map(
        on_device,
        mesh=fine,
        in_specs=(
            P(DP, BLK, None),
            P(DP, BLK, None),
            P(DP, BLK),
            P(DP, BLK),
            P(),
            P(),
            P(),
        ),
        out_specs=(P(), P(), P()),
        check_vma=False,
    )
```

```python
import functools

import jax
import jax.numpy as jnp
from jax import lax
from jax.experimental import pallas as pl
from jax.experimental.pallas import tpu as pltpu
from jax.sharding import Mesh
from jax.sharding import PartitionSpec as P

EXCLUDED = -1e30
BLK = ("yh", "z", "c")
DP = ("x", "yl")
META = 16
LIMIT, BIG = 6 << 20, 8 << 20

f32, bf16 = jnp.float32, jnp.bfloat16


def dot(a, b, ca, cb):
    return lax.dot_general(a, b, (((ca,), (cb,)), ((), ())), preferred_element_type=f32)


def shift(x, axis, by):
    n = lax.axis_size(axis)
    return lax.ppermute(x, axis, [(i, (i + by) % n) for i in range(n)])


def split3(x):
    hi = lax.reduce_precision(x, 8, 7)
    rest = x - hi
    mid = lax.reduce_precision(rest, 8, 7)
    return hi, mid, rest - mid


def join_meta(meta, at, scales):
    v = meta.astype(f32)
    left = sum(v[at + 2 * k : at + 2 * k + 1, :] * s for k, s in enumerate(scales))
    right = sum(v[at + 2 * k + 1 : at + 2 * k + 2, :128] * s for k, s in enumerate(scales))
    return jnp.concatenate([left, right], axis=1)


def ids_of(meta):
    return join_meta(meta, 0, (65536.0, 256.0, 1.0))


def corrections_of(meta):
    return join_meta(meta, 6, (1.0, 1.0, 1.0))


def eye():
    return lax.broadcasted_iota(jnp.int32, (128, 128), 0) == lax.broadcasted_iota(jnp.int32, (128, 128), 1)


def down(row):
    return jnp.sum(jnp.where(eye(), row, 0.0), axis=1, keepdims=True)


def across(col):
    return jnp.sum(jnp.where(eye(), col, 0.0), axis=0, keepdims=True)


def call(kernel, name, out_shape, *args, flops=0, scratch=(), limit=LIMIT, specs=None):
    size = sum(a.size * a.dtype.itemsize for a in (*args, *jax.tree.leaves(out_shape)))
    extra = {} if specs is None else {"in_specs": specs}
    return pl.pallas_call(
        kernel,
        out_shape=out_shape,
        scratch_shapes=scratch,
        compiler_params=pltpu.CompilerParams(vmem_limit_bytes=limit),
        cost_estimate=pl.CostEstimate(flops=max(flops, 1), bytes_accessed=size, transcendentals=0),
        name=name,
        **extra,
    )(*args)


def prep_kernel(rows, b0, b1, b2, q_ref, qt_ref, id_ref):
    full = rows + META
    for k, (b, at) in enumerate(((b0, 0), (b1, 0), (b2, 0), (b2, full))):
        v = b[at : at + rows, :].astype(f32)
        q_ref[k * rows : (k + 1) * rows, :] = (v * 0.0625).astype(bf16)
        qt_ref[:, k * rows : (k + 1) * rows] = jnp.transpose(v).astype(bf16)
        ids = ids_of(b[at + rows : at + full, :])
        for j in range(rows // 128):
            id_ref[k * rows + j * 128 : k * rows + (j + 1) * 128, :] = jnp.broadcast_to(
                down(ids[:, j * 128 : (j + 1) * 128]), (128, 128)
            )


def prep(own, near, other):
    rows, wide = own.shape[0] - META, own.shape[1]
    out = (
        jax.ShapeDtypeStruct((4 * rows, wide), bf16),
        jax.ShapeDtypeStruct((wide, 4 * rows), bf16),
        jax.ShapeDtypeStruct((4 * rows, 128), f32),
    )
    return call(functools.partial(prep_kernel, rows), "prep", out, own, near, other, flops=10**8)


def step_kernel(first, nb, rows, tm, *refs):
    q_ref, id_ref = refs[:2]
    blocks = refs[2 : 2 + nb]
    at = 2 + nb
    if not first:
        lse_in = refs[at]
        at += 1
    p_ref, md_ref, lse_ref, items = refs[at:]
    for k, b in enumerate(blocks):
        items[k * rows : (k + 1) * rows, :] = b[:rows, :]
    metas = [b[rows : rows + META, :] for b in blocks]
    col_ids = jnp.concatenate([ids_of(m) for m in metas], axis=1)
    corr = jnp.concatenate([corrections_of(m) for m in metas], axis=1)
    cols = nb * rows

    def tile(t, carry):
        at = pl.ds(pl.multiple_of(t * tm, tm), tm)
        s = dot(q_ref[at, :], items[...], 1, 1) - corr
        dup = jnp.concatenate([id_ref[at, :]] * (cols // 128), axis=1) == col_ids
        if first:
            row = lax.broadcasted_iota(jnp.int32, (tm, cols), 0) + t * tm
            dup = dup & (row != lax.broadcasted_iota(jnp.int32, (tm, cols), 1))
        s = jnp.where(dup, EXCLUDED, s)
        m = jnp.max(s, axis=1, keepdims=True)
        p = jnp.exp(s - m)
        part = m + jnp.log(jnp.sum(p, axis=1, keepdims=True))
        p_ref[at, :] = p.astype(bf16)
        for j in range(tm // 128):
            sub = slice(j * 128, (j + 1) * 128)
            lane = pl.ds(pl.multiple_of(t * tm + j * 128, 128), 128)
            md_ref[:, lane] = across(m[sub])
            lse = across(part[sub])
            lse_ref[:, lane] = lse if first else log_add(lse_in[:, lane], lse)
        return carry

    lax.fori_loop(0, q_ref.shape[0] // tm, tile, 0)


def step(q, ids, blocks, lse, tm=256):
    n, wide = q.shape
    nb, rows = len(blocks), blocks[0].shape[0] - META
    row = jax.ShapeDtypeStruct((1, n), f32)
    return call(
        functools.partial(step_kernel, lse is None, nb, rows, tm),
        "scores",
        (jax.ShapeDtypeStruct((n, nb * rows), bf16), row, row),
        q,
        ids,
        *blocks,
        *(() if lse is None else (lse,)),
        flops=4 * n * nb * rows * wide,
        scratch=[pltpu.VMEM((nb * rows, wide), bf16)],
    )


def back_kernel(qt_ref, p_ref, md_ref, lse_ref, *outs):
    w = jnp.exp(md_ref[...] - lse_ref[...])
    qw = (qt_ref[...].astype(f32) * w).astype(bf16)
    t = dot(qw, p_ref[...], 1, 0)
    rows = t.shape[1] // len(outs)
    for k, o in enumerate(outs):
        o[...] = t[:, k * rows : (k + 1) * rows].astype(o.dtype)


def back(qt, p, md, lse, nb, dtype):
    wide, n = qt.shape
    rows = p.shape[1] // nb
    out = [jax.ShapeDtypeStruct((wide, rows), dtype)] * nb
    return call(back_kernel, "back", out, qt, p, md, lse, flops=4 * n * nb * rows * wide)


def sums_kernel(groups, rows, *refs):
    n_p, n_b = len(groups), sum(groups)
    ps, mds = refs[:n_p], refs[n_p : 2 * n_p]
    blocks = refs[2 * n_p : 2 * n_p + n_b]
    lse_ref, pos_ref, keep_ref, send_ref, items = refs[2 * n_p + n_b :]
    for k, b in enumerate(blocks):
        items[k * rows : (k + 1) * rows, :] = b[:rows, :]
    half = 2 * rows
    for r in range(2 * half // 128):
        at = slice(r * 128, (r + 1) * 128)
        lse = lse_ref[:, at]
        o, first = None, 0
        for p, md, nb in zip(ps, mds, groups):
            part = dot(p[at, :], items[first : first + nb * rows, :], 1, 0) * down(jnp.exp(md[:, at] - lse))
            o = part if o is None else o + part
            first += nb * rows
        if r * 128 < half:
            keep_ref[at, :] = o
        else:
            send_ref[r * 128 - half : (r + 1) * 128 - half, :] = o
    loss = jnp.sum(lse_ref[:, :rows], axis=1, keepdims=True) - pos_ref[...]
    for ref in (keep_ref, send_ref):
        ref[half : half + 8, :] = jnp.broadcast_to(loss, (8, ref.shape[1]))


def sums(ps, mds, blocks, groups, lse, pos):
    rows, wide = blocks[0].shape[0] - META, blocks[0].shape[1]
    out = [jax.ShapeDtypeStruct((2 * rows + 8, wide), f32)] * 2
    return call(
        functools.partial(sums_kernel, groups, rows),
        "sums",
        out,
        *ps,
        *mds,
        *blocks,
        lse,
        pos,
        flops=2 * 4 * rows * len(blocks) * rows * wide,
        scratch=[pltpu.VMEM((len(blocks) * rows, wide), bf16)],
        limit=BIG,
    )


def log_add(a, b):
    top = jnp.maximum(a, b)
    return top + jnp.log(jnp.exp(a - top) + jnp.exp(b - top))


def tower_kernel(core_ref, own_ref, up_ref, dn_ref, qt_ref, feats_ref, tq_ref, keep_ref, give_ref):
    total = own_ref[...] + up_ref[...].astype(f32) + dn_ref[...].astype(f32)
    grad = ((total - qt_ref[...].astype(f32)) * 0.0625).astype(bf16)
    tower = dot(grad, feats_ref[...], 1, 0)
    first = core_ref[0] == 0

    def put(ref, v):
        for r in range(v.shape[0] // 128):
            for l in range(v.shape[1] // 128):
                ref[r * (v.shape[1] // 128) + l, :, :] = v[r * 128 : (r + 1) * 128, l * 128 : (l + 1) * 128]

    @pl.when(first)
    def _():
        put(keep_ref, tq_ref[...])
        put(give_ref, tower)

    @pl.when(jnp.logical_not(first))
    def _():
        put(keep_ref, tower)
        put(give_ref, tq_ref[...])


def finish_kernel(core_ref, mine_ref, other_ref, gq_ref, gi_ref):
    across_tiles = gq_ref.shape[0] // 128

    def put(ref, src):
        for k in range(src.shape[0]):
            r, l = divmod(k, across_tiles)
            ref[l * 128 : (l + 1) * 128, r * 128 : (r + 1) * 128] = jnp.transpose(src[k, :, :].astype(f32))

    first = core_ref[0] == 0

    @pl.when(first)
    def _():
        put(gq_ref, mine_ref)
        put(gi_ref, other_ref)

    @pl.when(jnp.logical_not(first))
    def _():
        put(gq_ref, other_ref)
        put(gi_ref, mine_ref)


def on_device(query_feats, item_feats, item_ids, bucket_ids, bucket_logq, query_tower, item_tower):
    query_input, item_input = query_feats[0], item_feats[0]
    rows, feats = query_input.shape
    wide = query_tower.shape[1]
    own_ids, own_buckets = item_ids[0], bucket_ids[0]
    scaling = 1.0 / 16.0
    buckets = jnp.arange(bucket_logq.shape[0], dtype=jnp.int32)
    correction = jnp.sum(jnp.where(own_buckets[:, None] == buckets[None, :], bucket_logq[None, :], 0.0), axis=1)
    pieces = [own_ids // 65536, (own_ids // 256) % 256, own_ids % 256]
    pieces = [p.astype(f32) for p in pieces] + list(split3(correction))
    meta = jnp.stack([jnp.pad(p, (0, 512 - rows)) for p in pieces]).reshape(12, 256)
    meta = jnp.pad(meta, ((0, META - 12), (0, 0))).astype(bf16)
    item_vecs = jnp.dot(item_input, item_tower, preferred_element_type=f32).astype(bf16)
    query_vecs = jnp.dot(query_input, query_tower, preferred_element_type=f32).astype(bf16)
    item_block = jnp.concatenate([item_vecs, meta])
    query_block = jnp.concatenate([query_vecs, meta])
    positive = jnp.sum(query_vecs.astype(f32) * item_vecs.astype(f32)) * scaling - jnp.sum(correction)
    core = lax.axis_index("c").reshape(1)

    near = shift(query_block, "yh", 1)
    up, dn = [item_block], [item_block]
    for k in range(1, 5):
        up.append(shift(up[-1], "z", 1))
        if k < 4:
            dn.append(shift(dn[-1], "z", -1))
    other = shift(jnp.concatenate([query_block, near]), "c", 1)
    q, qt, ids = prep(query_block, near, other)
    groups = [[item_block]] + [[up[k], dn[k]] for k in (1, 2, 3)] + [[up[4]]]
    ps, mds, lse = [], [], None
    for blocks in groups:
        p, md, lse = step(q, ids, blocks, lse)
        ps.append(p)
        mds.append(md)

    def swapped(row, bit):
        return jnp.concatenate([row[:, (k ^ bit) * rows : ((k ^ bit) + 1) * rows] for k in range(4)], axis=1)

    lse = log_add(lse, swapped(shift(lse, "c", 1), 2))
    lse = log_add(lse, swapped(shift(lse, "yh", 1), 1))

    ring_up = shift(back(qt, ps[4], mds[4], lse, 1, bf16)[0], "z", 1)
    ring_dn = None
    for k in (3, 2, 1):
        t_up, t_dn = back(qt, ps[k], mds[k], lse, 2, f32)
        t_dn, t_up = t_up, t_dn
        ring_up = shift((ring_up.astype(f32) + t_up).astype(bf16), "z", 1)
        ring_dn = shift((t_dn if ring_dn is None else ring_dn.astype(f32) + t_dn).astype(bf16), "z", -1)
        if k == 3:
            flat = [b for blocks in groups for b in blocks]
            o_keep, o_send = sums(ps, mds, flat, [len(b) for b in groups], lse, positive.reshape(1, 1))
            o_2 = o_keep + shift(o_send, "c", 1)
    o_y = shift(o_2[rows : 2 * rows].astype(bf16), "yh", 1)
    t_own = back(qt, ps[0], mds[0], lse, 1, f32)[0]
    o = o_2[:rows] + o_y.astype(f32)
    query_grad = ((o - item_vecs.astype(f32)) * scaling).astype(bf16)
    tower_query = dot(query_grad, query_input, 0, 0)

    tiles = (wide // 128) * (feats // 128)
    whole = pl.BlockSpec(memory_space=pltpu.VMEM)
    smem = pl.BlockSpec(memory_space=pltpu.SMEM)
    out = [jax.ShapeDtypeStruct((tiles, 128, 128), f32)] * 2
    keep, give = call(
        tower_kernel, "towers", out, core, t_own, ring_up, ring_dn, qt[:, :rows], item_input, tower_query,
        flops=2 * rows * wide * feats, specs=[smem] + [whole] * 6,
    )
    plane = ("yh", "x", "yl")
    n, nz = lax.axis_size(plane), lax.axis_size("z")

    def with_loss(parts, loss):
        three = jnp.stack(split3(loss))
        under = jnp.broadcast_to(jnp.pad(three, (0, 5))[None, :, None], (parts.shape[0], 8, 128))
        return jnp.concatenate([parts.astype(bf16), under.astype(bf16)], axis=1)

    sent = with_loss(keep + shift(give, "c", 1), o_2[2 * rows, 0])
    total = jnp.sum(lax.all_to_all(sent, plane, 0, 0, tiled=True).astype(f32), axis=0)
    sent = with_loss(total[None, :128], jnp.sum(total[128:131, 0]))
    sent = jnp.broadcast_to(sent, (nz, *sent.shape[1:]))
    total = jnp.sum(lax.all_to_all(sent, "z", 0, 0, tiled=True).astype(f32), axis=0)
    loss = jnp.sum(total[128:131, 0])
    mine = jnp.broadcast_to(total[:128].astype(bf16)[None], (n, 128, 128))
    mine = lax.all_to_all(mine, plane, 0, 0, tiled=True)
    rest = shift(mine, "c", 1)
    out = [jax.ShapeDtypeStruct((feats, wide), f32)] * 2
    grad_query, grad_item = call(finish_kernel, "finish", out, core, mine, rest, specs=[smem, whole, whole])
    count = lax.axis_size(BLK) * rows * lax.axis_size(DP)
    return (grad_query, grad_item, loss / count)


def solution(mesh):
    fine = Mesh(mesh.devices.reshape(2, 8, 2, 4, 2), ("yh", "z", "c", "x", "yl"))
    return jax.shard_map(
        on_device,
        mesh=fine,
        in_specs=(
            P(DP, BLK, None),
            P(DP, BLK, None),
            P(DP, BLK),
            P(DP, BLK),
            P(),
            P(),
            P(),
        ),
        out_specs=(P(), P(), P()),
        check_vma=False,
    )
```

```python
import functools

import jax
import jax.numpy as jnp
from jax import lax
from jax.experimental import pallas as pl
from jax.experimental.pallas import tpu as pltpu
from jax.sharding import Mesh
from jax.sharding import PartitionSpec as P

EXCLUDED = -1e30
BLK = ("yh", "z", "c")
DP = ("x", "yl")
META = 16
LIMIT, BIG, HUGE = 6 << 20, 8 << 20, 60 << 20

f32, bf16 = jnp.float32, jnp.bfloat16


def dot(a, b, ca, cb):
    return lax.dot_general(a, b, (((ca,), (cb,)), ((), ())), preferred_element_type=f32)


def shift(x, axis, by):
    n = lax.axis_size(axis)
    return lax.ppermute(x, axis, [(i, (i + by) % n) for i in range(n)])


def split3(x):
    hi = x.astype(bf16).astype(f32)
    mid = (x - hi).astype(bf16).astype(f32)
    return hi, mid, x - hi - mid


def join_meta(meta, at, scales):
    v = meta.astype(f32)
    left = sum(v[at + 2 * k : at + 2 * k + 1, :] * s for k, s in enumerate(scales))
    right = sum(v[at + 2 * k + 1 : at + 2 * k + 2, :128] * s for k, s in enumerate(scales))
    return jnp.concatenate([left, right], axis=1)


def ids_of(meta):
    return join_meta(meta, 0, (65536.0, 256.0, 1.0))


def corrections_of(meta):
    return join_meta(meta, 6, (1.0, 1.0, 1.0))


def eye():
    return lax.broadcasted_iota(jnp.int32, (128, 128), 0) == lax.broadcasted_iota(jnp.int32, (128, 128), 1)


def down(row):
    return jnp.sum(jnp.where(eye(), row, 0.0), axis=1, keepdims=True)


def across(col):
    return jnp.sum(jnp.where(eye(), col, 0.0), axis=0, keepdims=True)


def call(kernel, out_shape, *args, flops=0, scratch=(), limit=LIMIT, specs=None):
    size = sum(a.size * a.dtype.itemsize for a in (*args, *jax.tree.leaves(out_shape)))
    extra = {} if specs is None else {"in_specs": specs}
    return pl.pallas_call(
        kernel,
        out_shape=out_shape,
        scratch_shapes=scratch,
        compiler_params=pltpu.CompilerParams(vmem_limit_bytes=limit),
        cost_estimate=pl.CostEstimate(flops=max(flops, 1), bytes_accessed=size, transcendentals=0),
        **extra,
    )(*args)


def embed_kernel(core_ref, *refs):
    sources, refs = refs[:7], refs[7:]
    q_out, i_out, pos_ref, *scratch = refs
    meta, sems, buffers = scratch[0], scratch[1], scratch[2:]
    copies = [pltpu.make_async_copy(s, d, sems.at[k]) for k, (s, d) in enumerate(zip(sources, buffers))]
    for c in copies:
        c.start()
    ids_ref, buckets_ref, logq_ref, item_ref, item_tower, query_ref, query_tower = buffers
    rows = item_ref.shape[0]
    for c in copies[:3]:
        c.wait()
    logq = logq_ref[...]
    nb = logq.shape[1]
    table = jnp.concatenate([down(logq[:, k : k + 128]) for k in range(0, nb, 128)], axis=0)
    hit = lax.broadcasted_iota(jnp.int32, (nb, rows), 0) == buckets_ref[...]
    correction = jnp.sum(jnp.where(hit, table, 0.0), axis=0, keepdims=True)
    ids = ids_ref[...]
    parts = [(ids >> 16).astype(f32), ((ids >> 8) & 255).astype(f32), (ids & 255).astype(f32)]
    meta[...] = jnp.zeros_like(meta)
    for k, v in enumerate((*parts, *split3(correction))):
        meta[2 * k : 2 * k + 1, :] = v[:, :256]
        meta[2 * k + 1 : 2 * k + 2, : rows - 256] = v[:, 256:]
    low = meta[...].astype(bf16)
    i_out[rows:, :] = low
    q_out[rows:, :] = low
    for c in copies[3:5]:
        c.wait()
    i_out[:rows, :] = dot(item_ref[...], item_tower[...], 1, 0).astype(bf16)
    for c in copies[5:]:
        c.wait()
    vecs = dot(query_ref[...], query_tower[...], 1, 0).astype(bf16)
    q_out[:rows, :] = vecs
    product = vecs.astype(f32) * i_out[:rows, :].astype(f32) * 0.0625
    total = jnp.sum(jnp.sum(product, axis=0, keepdims=True), axis=1, keepdims=True)
    pos_ref[...] = total - jnp.sum(correction, axis=1, keepdims=True)


def lse_kernel(bit, rows, mine_ref, other_ref, out_ref):
    for k in range(4):
        at, of = slice(k * rows, (k + 1) * rows), slice((k ^ bit) * rows, ((k ^ bit) + 1) * rows)
        out_ref[:, at] = log_add(mine_ref[:, at], other_ref[:, of])


def loss_rows(loss):
    row = lax.broadcasted_iota(jnp.int32, (8, 128), 0)
    hi, mid, lo = split3(loss)
    return jnp.where(row == 0, hi, jnp.where(row == 1, mid, jnp.where(row == 2, lo, 0.0)))


def pack_kernel(keep_ref, other_ref, loss_ref, out_ref):
    low = loss_rows(loss_ref[:1, :128]).astype(bf16)
    for k in range(keep_ref.shape[0]):
        out_ref[k, :128, :] = (keep_ref[k, :, :] + other_ref[k, :, :]).astype(bf16)
        out_ref[k, 128:, :] = low


def plane_kernel(in_ref, out_ref):
    total = sum(in_ref[k, :, :].astype(f32) for k in range(in_ref.shape[0]))
    low = loss_rows(jnp.sum(total[128:, :], axis=0, keepdims=True)).astype(bf16)
    top = total[:128, :].astype(bf16)
    for k in range(out_ref.shape[0]):
        out_ref[k, :128, :] = top
        out_ref[k, 128:, :] = low


def z_kernel(count, in_ref, out_ref, loss_ref):
    total = sum(in_ref[k, :, :].astype(f32) for k in range(in_ref.shape[0]))
    top = total[:128, :].astype(bf16)
    for k in range(out_ref.shape[0]):
        out_ref[k, :, :] = top
    loss_ref[...] = jnp.sum(total[128:, :], axis=0, keepdims=True) * (1.0 / count)


def prep_kernel(rows, b0, b1, b2, q_ref, qt_ref, id_ref):
    full = rows + META
    for k, (b, at) in enumerate(((b0, 0), (b1, 0), (b2, 0), (b2, full))):
        v = b[at : at + rows, :].astype(f32)
        q_ref[k * rows : (k + 1) * rows, :] = (v * 0.0625).astype(bf16)
        qt_ref[:, k * rows : (k + 1) * rows] = jnp.transpose(v).astype(bf16)
        ids = ids_of(b[at + rows : at + full, :])
        for j in range(rows // 128):
            id_ref[k * rows + j * 128 : k * rows + (j + 1) * 128, :] = jnp.broadcast_to(
                down(ids[:, j * 128 : (j + 1) * 128]), (128, 128)
            )


def prep(own, near, other):
    rows, wide = own.shape[0] - META, own.shape[1]
    out = (
        jax.ShapeDtypeStruct((4 * rows, wide), bf16),
        jax.ShapeDtypeStruct((wide, 4 * rows), bf16),
        jax.ShapeDtypeStruct((4 * rows, 128), f32),
    )
    return call(functools.partial(prep_kernel, rows), out, own, near, other, flops=10**8)


def step_kernel(first, nb, rows, tm, *refs):
    q_ref, id_ref = refs[:2]
    blocks = refs[2 : 2 + nb]
    at = 2 + nb
    if not first:
        lse_in = refs[at]
        at += 1
    p_ref, md_ref, lse_ref, items = refs[at:]
    for k, b in enumerate(blocks):
        items[k * rows : (k + 1) * rows, :] = b[:rows, :]
    metas = [b[rows : rows + META, :] for b in blocks]
    col_ids = jnp.concatenate([ids_of(m) for m in metas], axis=1)
    corr = jnp.concatenate([corrections_of(m) for m in metas], axis=1)
    cols = nb * rows

    def tile(t, carry):
        at = pl.ds(pl.multiple_of(t * tm, tm), tm)
        s = dot(q_ref[at, :], items[...], 1, 1) - corr
        dup = jnp.concatenate([id_ref[at, :]] * (cols // 128), axis=1) == col_ids
        if first:
            row = lax.broadcasted_iota(jnp.int32, (tm, cols), 0) + t * tm
            dup = dup & (row != lax.broadcasted_iota(jnp.int32, (tm, cols), 1))
        s = jnp.where(dup, EXCLUDED, s)
        m = jnp.max(s, axis=1, keepdims=True)
        p = jnp.exp(s - m)
        part = m + jnp.log(jnp.sum(p, axis=1, keepdims=True))
        p_ref[at, :] = p.astype(bf16)
        for j in range(tm // 128):
            sub = slice(j * 128, (j + 1) * 128)
            lane = pl.ds(pl.multiple_of(t * tm + j * 128, 128), 128)
            md_ref[:, lane] = across(m[sub])
            lse = across(part[sub])
            lse_ref[:, lane] = lse if first else log_add(lse_in[:, lane], lse)
        return carry

    lax.fori_loop(0, q_ref.shape[0] // tm, tile, 0, unroll=3)


def step(q, ids, blocks, lse, tm=256):
    n, wide = q.shape
    nb, rows = len(blocks), blocks[0].shape[0] - META
    row = jax.ShapeDtypeStruct((1, n), f32)
    return call(
        functools.partial(step_kernel, lse is None, nb, rows, tm),
        (jax.ShapeDtypeStruct((n, nb * rows), bf16), row, row),
        q,
        ids,
        *blocks,
        *(() if lse is None else (lse,)),
        flops=4 * n * nb * rows * wide,
        scratch=[pltpu.VMEM((nb * rows, wide), bf16)],
    )


def back_kernel(qt_ref, p_ref, md_ref, lse_ref, *outs):
    w = jnp.exp(md_ref[...] - lse_ref[...])
    qw = (qt_ref[...].astype(f32) * w).astype(bf16)
    t = dot(qw, p_ref[...], 1, 0)
    rows = t.shape[1] // len(outs)
    for k, o in enumerate(outs):
        o[...] = t[:, k * rows : (k + 1) * rows].astype(o.dtype)


def back(qt, p, md, lse, *dtypes):
    wide, n = qt.shape
    rows = p.shape[1] // len(dtypes)
    out = [jax.ShapeDtypeStruct((wide, rows), dtype) for dtype in dtypes]
    return call(back_kernel, out, qt, p, md, lse, flops=4 * n * p.shape[1] * wide)


def sums_kernel(groups, rows, *refs):
    n_p, n_b = len(groups), sum(groups)
    ps, mds = refs[:n_p], refs[n_p : 2 * n_p]
    blocks = refs[2 * n_p : 2 * n_p + n_b]
    lse_ref, pos_ref, keep_ref, send_ref, items = refs[2 * n_p + n_b :]
    for k, b in enumerate(blocks):
        items[k * rows : (k + 1) * rows, :] = b[:rows, :]
    half = 2 * rows
    for r in range(2 * half // 128):
        at = slice(r * 128, (r + 1) * 128)
        lse = lse_ref[:, at]
        o, first = None, 0
        for p, md, nb in zip(ps, mds, groups):
            part = dot(p[at, :], items[first : first + nb * rows, :], 1, 0) * down(jnp.exp(md[:, at] - lse))
            o = part if o is None else o + part
            first += nb * rows
        if r * 128 < half:
            keep_ref[at, :] = o
        else:
            send_ref[r * 128 - half : (r + 1) * 128 - half, :] = o
    loss = jnp.sum(lse_ref[:, :rows], axis=1, keepdims=True) - pos_ref[...]
    for ref in (keep_ref, send_ref):
        ref[half : half + 8, :] = jnp.broadcast_to(loss, (8, ref.shape[1]))


def sums(ps, mds, blocks, groups, lse, pos):
    rows, wide = blocks[0].shape[0] - META, blocks[0].shape[1]
    out = [jax.ShapeDtypeStruct((2 * rows + 8, wide), f32)] * 2
    return call(
        functools.partial(sums_kernel, groups, rows),
        out,
        *ps,
        *mds,
        *blocks,
        lse,
        pos,
        flops=2 * 4 * rows * len(blocks) * rows * wide,
        scratch=[pltpu.VMEM((len(blocks) * rows, wide), bf16)],
        limit=BIG,
    )


def log_add(a, b):
    top = jnp.maximum(a, b)
    return top + jnp.log(jnp.exp(a - top) + jnp.exp(b - top))


def tower_kernel(core_ref, own_ref, up_ref, dn_ref, qt_ref, feats_ref, tq_ref, keep_ref, give_ref):
    total = own_ref[...] + up_ref[...].astype(f32) + dn_ref[...].astype(f32)
    grad = ((total - qt_ref[...].astype(f32)) * 0.0625).astype(bf16)
    tower = dot(grad, feats_ref[...], 1, 0)
    first = core_ref[0] == 0

    def put(ref, v):
        for r in range(v.shape[0] // 128):
            for l in range(v.shape[1] // 128):
                ref[r * (v.shape[1] // 128) + l, :, :] = v[r * 128 : (r + 1) * 128, l * 128 : (l + 1) * 128]

    @pl.when(first)
    def _():
        put(keep_ref, tq_ref[...])
        put(give_ref, tower)

    @pl.when(jnp.logical_not(first))
    def _():
        put(keep_ref, tower)
        put(give_ref, tq_ref[...])


def finish_kernel(core_ref, mine_ref, other_ref, gq_ref, gi_ref):
    across_tiles = gq_ref.shape[0] // 128

    def put(ref, src):
        for k in range(src.shape[0]):
            r, l = divmod(k, across_tiles)
            ref[l * 128 : (l + 1) * 128, r * 128 : (r + 1) * 128] = jnp.transpose(src[k, :, :].astype(f32))

    first = core_ref[0] == 0

    @pl.when(first)
    def _():
        put(gq_ref, mine_ref)
        put(gi_ref, other_ref)

    @pl.when(jnp.logical_not(first))
    def _():
        put(gq_ref, other_ref)
        put(gi_ref, mine_ref)


def train_step(query_feats, item_feats, item_ids, bucket_ids, bucket_logq, query_tower, item_tower):
    query_input, item_input = query_feats[0], item_feats[0]
    rows, feats = query_input.shape
    wide = query_tower.shape[1]
    scaling = 1.0 / 16.0
    whole = pl.BlockSpec(memory_space=pltpu.VMEM)
    smem = pl.BlockSpec(memory_space=pltpu.SMEM)
    core = lax.axis_index("c").reshape(1)
    block = jax.ShapeDtypeStruct((rows + META, wide), bf16)
    sources = (item_ids, bucket_ids, bucket_logq.reshape(1, -1), item_input, item_tower, query_input, query_tower)
    query_block, item_block, positive = call(
        embed_kernel, (block, block, jax.ShapeDtypeStruct((1, 1), f32)), core, *sources,
        flops=4 * rows * feats * wide, specs=[smem] + [pl.BlockSpec(memory_space=pl.ANY)] * 7, limit=HUGE,
        scratch=[pltpu.VMEM((META, wide), f32), pltpu.SemaphoreType.DMA((7,))]
        + [pltpu.VMEM(a.shape, a.dtype) for a in sources],
    )

    up, dn = [item_block], [item_block]

    def ring(*after):
        u, d, _ = lax.optimization_barrier((up[-1], dn[-1], after))
        k = len(up)
        up.append(shift(u, "z", 1))
        if k < 4:
            dn.append(shift(d, "z", -1))

    ring()
    near = shift(query_block, "yh", 1)
    ring()
    other = shift(jnp.concatenate([query_block, near]), "c", 1)
    q, qt, ids = prep(query_block, near, other)
    ring(ids)
    ps, mds, lse = [], [], None
    for k in range(5):
        p, md, lse = step(q, ids, [up[k]] if k in (0, 4) else [up[k], dn[k]], lse)
        ps.append(p)
        mds.append(md)
        if k == 1:
            ring(lse)
    groups = [[item_block]] + [[up[k], dn[k]] for k in (1, 2, 3)] + [[up[4]]]

    row = jax.ShapeDtypeStruct(lse.shape, f32)
    lse = call(functools.partial(lse_kernel, 2, rows), row, lse, shift(lse, "c", 1))
    lse = call(functools.partial(lse_kernel, 1, rows), row, lse, shift(lse, "yh", 1))

    ring_up = shift(back(qt, ps[4], mds[4], lse, bf16)[0], "z", 1)
    ring_dn = None
    for k in (3, 2, 1):
        t_dn, t_up = back(qt, ps[k], mds[k], lse, bf16 if k == 3 else f32, f32)
        ring_up = shift((ring_up.astype(f32) + t_up).astype(bf16), "z", 1)
        ring_dn = t_dn if k == 3 else (ring_dn.astype(f32) + t_dn).astype(bf16)
        ring_dn = shift(ring_dn, "z", -1)
    t_own = back(qt, ps[0], mds[0], lse, f32)[0]
    flat = [b for blocks in groups for b in blocks]
    o_keep, o_send = sums(ps, mds, flat, [len(b) for b in groups], lse, positive)
    o_2 = o_keep + shift(o_send, "c", 1)
    o_y = shift(o_2[rows : 2 * rows].astype(bf16), "yh", 1)
    o = o_2[:rows] + o_y.astype(f32)
    query_grad = ((o - item_block[:rows].astype(f32)) * scaling).astype(bf16)
    tower_query = dot(query_grad, query_input, 0, 0)

    tiles = (wide // 128) * (feats // 128)
    out = [jax.ShapeDtypeStruct((tiles, 128, 128), f32)] * 2
    keep, give = call(
        tower_kernel, out, core, t_own, ring_up, ring_dn, qt[:, :rows], item_input, tower_query,
        flops=2 * rows * wide * feats, specs=[smem] + [whole] * 6,
    )
    plane = ("yh", "x", "yl")
    n, nz = lax.axis_size(plane), lax.axis_size("z")
    count = lax.axis_size(BLK) * rows * lax.axis_size(DP)
    sent = jax.ShapeDtypeStruct((n, 136, 128), bf16)
    sent = call(pack_kernel, sent, keep, shift(give, "c", 1), o_2[2 * rows :])
    got = lax.all_to_all(sent, plane, 0, 0, tiled=True)
    sent = call(plane_kernel, jax.ShapeDtypeStruct((nz, 136, 128), bf16), got)
    got = lax.all_to_all(sent, "z", 0, 0, tiled=True)
    out = (jax.ShapeDtypeStruct((n, 128, 128), bf16), jax.ShapeDtypeStruct((1, 128), f32))
    mine, loss = call(functools.partial(z_kernel, count), out, got)
    mine = lax.all_to_all(mine, plane, 0, 0, tiled=True)
    rest = shift(mine, "c", 1)
    out = [jax.ShapeDtypeStruct((feats, wide), f32)] * 2
    grad_query, grad_item = call(finish_kernel, out, core, mine, rest, specs=[smem, whole, whole])
    return (grad_query, grad_item, loss[0, 0])


def solution(mesh):
    fine = Mesh(mesh.devices.reshape(2, 8, 2, 4, 2), ("yh", "z", "c", "x", "yl"))
    return jax.shard_map(
        train_step,
        mesh=fine,
        in_specs=(
            P(DP, BLK, None),
            P(DP, BLK, None),
            P(DP, BLK),
            P(DP, BLK),
            P(),
            P(),
            P(),
        ),
        out_specs=(P(), P(), P()),
        check_vma=False,
    )
```

```python
import functools

import jax
import jax.numpy as jnp
from jax import lax
from jax.experimental import pallas as pl
from jax.experimental.pallas import tpu as pltpu
from jax.sharding import Mesh
from jax.sharding import PartitionSpec as P

EXCLUDED = -1e30
BLK = ("yh", "z", "c")
DP = ("x", "yl")
META = 16
LIMIT, BIG, HUGE = 6 << 20, 8 << 20, 60 << 20

f32, bf16 = jnp.float32, jnp.bfloat16


def dot(a, b, ca, cb):
    return lax.dot_general(a, b, (((ca,), (cb,)), ((), ())), preferred_element_type=f32)


def shift(x, axis, by):
    n = lax.axis_size(axis)
    return lax.ppermute(x, axis, [(i, (i + by) % n) for i in range(n)])


def split3(x):
    hi = x.astype(bf16).astype(f32)
    mid = (x - hi).astype(bf16).astype(f32)
    return hi, mid, x - hi - mid


def join_meta(meta, at, scales):
    v = meta.astype(f32)
    left = sum(v[at + 2 * k : at + 2 * k + 1, :] * s for k, s in enumerate(scales))
    right = sum(v[at + 2 * k + 1 : at + 2 * k + 2, :128] * s for k, s in enumerate(scales))
    return jnp.concatenate([left, right], axis=1)


def ids_of(meta):
    return join_meta(meta, 0, (65536.0, 256.0, 1.0))


def corrections_of(meta):
    return join_meta(meta, 6, (1.0, 1.0, 1.0))


def eye():
    return lax.broadcasted_iota(jnp.int32, (128, 128), 0) == lax.broadcasted_iota(jnp.int32, (128, 128), 1)


def down(row):
    return jnp.sum(jnp.where(eye(), row, 0.0), axis=1, keepdims=True)


def across(col):
    return jnp.sum(jnp.where(eye(), col, 0.0), axis=0, keepdims=True)


def call(kernel, out_shape, *args, flops=0, scratch=(), limit=LIMIT, specs=None):
    size = sum(a.size * a.dtype.itemsize for a in (*args, *jax.tree.leaves(out_shape)))
    extra = {} if specs is None else {"in_specs": specs}
    return pl.pallas_call(
        kernel,
        out_shape=out_shape,
        scratch_shapes=scratch,
        compiler_params=pltpu.CompilerParams(vmem_limit_bytes=limit),
        cost_estimate=pl.CostEstimate(flops=max(flops, 1), bytes_accessed=size, transcendentals=0),
        **extra,
    )(*args)


def embed_kernel(core_ref, *refs):
    sources, refs = refs[:7], refs[7:]
    q_out, i_out, pos_ref, *scratch = refs
    meta, sems, buffers = scratch[0], scratch[1], scratch[2:]
    copies = [pltpu.make_async_copy(s, d, sems.at[k]) for k, (s, d) in enumerate(zip(sources, buffers))]
    for c in copies:
        c.start()
    ids_ref, buckets_ref, logq_ref, item_ref, item_tower, query_ref, query_tower = buffers
    rows = item_ref.shape[0]
    for c in copies[:3]:
        c.wait()
    logq = logq_ref[...]
    nb = logq.shape[1]
    table = jnp.concatenate([down(logq[:, k : k + 128]) for k in range(0, nb, 128)], axis=0)
    hit = lax.broadcasted_iota(jnp.int32, (nb, rows), 0) == buckets_ref[...]
    correction = jnp.sum(jnp.where(hit, table, 0.0), axis=0, keepdims=True)
    ids = ids_ref[...]
    parts = [(ids >> 16).astype(f32), ((ids >> 8) & 255).astype(f32), (ids & 255).astype(f32)]
    meta[...] = jnp.zeros_like(meta)
    for k, v in enumerate((*parts, *split3(correction))):
        meta[2 * k : 2 * k + 1, :] = v[:, :256]
        meta[2 * k + 1 : 2 * k + 2, : rows - 256] = v[:, 256:]
    low = meta[...].astype(bf16)
    i_out[rows:, :] = low
    q_out[rows:, :] = low
    for c in copies[3:5]:
        c.wait()
    i_out[:rows, :] = dot(item_ref[...], item_tower[...], 1, 0).astype(bf16)
    for c in copies[5:]:
        c.wait()
    vecs = dot(query_ref[...], query_tower[...], 1, 0).astype(bf16)
    q_out[:rows, :] = vecs
    product = vecs.astype(f32) * i_out[:rows, :].astype(f32) * 0.0625
    total = jnp.sum(jnp.sum(product, axis=0, keepdims=True), axis=1, keepdims=True)
    pos_ref[...] = total - jnp.sum(correction, axis=1, keepdims=True)


def lse_kernel(bit, rows, mine_ref, other_ref, out_ref):
    for k in range(4):
        at, of = slice(k * rows, (k + 1) * rows), slice((k ^ bit) * rows, ((k ^ bit) + 1) * rows)
        out_ref[:, at] = log_add(mine_ref[:, at], other_ref[:, of])


def loss_rows(loss):
    row = lax.broadcasted_iota(jnp.int32, (8, 128), 0)
    hi, mid, lo = split3(loss)
    return jnp.where(row == 0, hi, jnp.where(row == 1, mid, jnp.where(row == 2, lo, 0.0)))


def pack_kernel(keep_ref, other_ref, loss_ref, out_ref):
    low = loss_rows(loss_ref[:1, :128]).astype(bf16)
    for k in range(keep_ref.shape[0]):
        out_ref[k, :128, :] = (keep_ref[k, :, :] + other_ref[k, :, :]).astype(bf16)
        out_ref[k, 128:, :] = low


def plane_kernel(in_ref, out_ref):
    total = sum(in_ref[k, :, :].astype(f32) for k in range(in_ref.shape[0]))
    low = loss_rows(jnp.sum(total[128:, :], axis=0, keepdims=True)).astype(bf16)
    top = total[:128, :].astype(bf16)
    for k in range(out_ref.shape[0]):
        out_ref[k, :128, :] = top
        out_ref[k, 128:, :] = low


def z_kernel(count, in_ref, out_ref, loss_ref):
    total = sum(in_ref[k, :, :].astype(f32) for k in range(in_ref.shape[0]))
    top = total[:128, :].astype(bf16)
    for k in range(out_ref.shape[0]):
        out_ref[k, :, :] = top
    loss_ref[...] = jnp.sum(total[128:, :], axis=0, keepdims=True) * (1.0 / count)


def fetch_kernel(a_ref, b_ref, a_out, b_out):
    a_out[...] = a_ref[...]
    b_out[...] = b_ref[...]


def prep_kernel(rows, b0, b2, q_ref, qt_ref, id_ref):
    full = rows + META
    for k, (b, at) in enumerate(((b0, 0), (b0, full), (b2, 0), (b2, full))):
        v = b[at : at + rows, :].astype(f32)
        q_ref[k * rows : (k + 1) * rows, :] = (v * 0.0625).astype(bf16)
        qt_ref[:, k * rows : (k + 1) * rows] = jnp.transpose(v).astype(bf16)
        ids = ids_of(b[at + rows : at + full, :])
        for j in range(rows // 128):
            id_ref[k * rows + j * 128 : k * rows + (j + 1) * 128, :] = jnp.broadcast_to(
                down(ids[:, j * 128 : (j + 1) * 128]), (128, 128)
            )


def prep(pair, other):
    rows, wide = pair.shape[0] // 2 - META, pair.shape[1]
    out = (
        jax.ShapeDtypeStruct((4 * rows, wide), bf16),
        jax.ShapeDtypeStruct((wide, 4 * rows), bf16),
        jax.ShapeDtypeStruct((4 * rows, 128), f32),
    )
    return call(functools.partial(prep_kernel, rows), out, pair, other, flops=10**8)


def step_kernel(first, nb, rows, tm, *refs):
    q_ref, id_ref = refs[:2]
    blocks = refs[2 : 2 + nb]
    at = 2 + nb
    if not first:
        lse_in = refs[at]
        at += 1
    p_ref, md_ref, lse_ref, items = refs[at:]
    for k, b in enumerate(blocks):
        items[k * rows : (k + 1) * rows, :] = b[:rows, :]
    metas = [b[rows : rows + META, :] for b in blocks]
    col_ids = jnp.concatenate([ids_of(m) for m in metas], axis=1)
    corr = jnp.concatenate([corrections_of(m) for m in metas], axis=1)
    cols = nb * rows

    def tile(t, carry):
        at = pl.ds(pl.multiple_of(t * tm, tm), tm)
        s = dot(q_ref[at, :], items[...], 1, 1) - corr
        dup = jnp.concatenate([id_ref[at, :]] * (cols // 128), axis=1) == col_ids
        if first:
            row = lax.broadcasted_iota(jnp.int32, (tm, cols), 0) + t * tm
            dup = dup & (row != lax.broadcasted_iota(jnp.int32, (tm, cols), 1))
        s = jnp.where(dup, EXCLUDED, s)
        m = jnp.max(s, axis=1, keepdims=True)
        p = jnp.exp(s - m)
        part = m + jnp.log(jnp.sum(p, axis=1, keepdims=True))
        p_ref[at, :] = p.astype(bf16)
        for j in range(tm // 128):
            sub = slice(j * 128, (j + 1) * 128)
            lane = pl.ds(pl.multiple_of(t * tm + j * 128, 128), 128)
            md_ref[:, lane] = across(m[sub])
            lse = across(part[sub])
            lse_ref[:, lane] = lse if first else log_add(lse_in[:, lane], lse)
        return carry

    lax.fori_loop(0, q_ref.shape[0] // tm, tile, 0, unroll=3)


def step(q, ids, blocks, lse, tm=256):
    n, wide = q.shape
    nb, rows = len(blocks), blocks[0].shape[0] - META
    row = jax.ShapeDtypeStruct((1, n), f32)
    return call(
        functools.partial(step_kernel, lse is None, nb, rows, tm),
        (jax.ShapeDtypeStruct((n, nb * rows), bf16), row, row),
        q,
        ids,
        *blocks,
        *(() if lse is None else (lse,)),
        flops=4 * n * nb * rows * wide,
        scratch=[pltpu.VMEM((nb * rows, wide), bf16)],
    )


def back_kernel(qt_ref, p_ref, md_ref, lse_ref, *outs):
    w = jnp.exp(md_ref[...] - lse_ref[...])
    qw = (qt_ref[...].astype(f32) * w).astype(bf16)
    t = dot(qw, p_ref[...], 1, 0)
    rows = t.shape[1] // len(outs)
    for k, o in enumerate(outs):
        o[...] = t[:, k * rows : (k + 1) * rows].astype(o.dtype)


def back(qt, p, md, lse, *dtypes):
    wide, n = qt.shape
    rows = p.shape[1] // len(dtypes)
    out = [jax.ShapeDtypeStruct((wide, rows), dtype) for dtype in dtypes]
    return call(back_kernel, out, qt, p, md, lse, flops=4 * n * p.shape[1] * wide)


def sums_kernel(groups, rows, *refs):
    n_p, n_b = len(groups), sum(groups)
    ps, mds = refs[:n_p], refs[n_p : 2 * n_p]
    blocks = refs[2 * n_p : 2 * n_p + n_b]
    lse_ref, pos_ref, keep_ref, send_ref, items = refs[2 * n_p + n_b :]
    for k, b in enumerate(blocks):
        items[k * rows : (k + 1) * rows, :] = b[:rows, :]
    half = 2 * rows
    for r in range(2 * half // 128):
        at = slice(r * 128, (r + 1) * 128)
        lse = lse_ref[:, at]
        o, first = None, 0
        for p, md, nb in zip(ps, mds, groups):
            part = dot(p[at, :], items[first : first + nb * rows, :], 1, 0) * down(jnp.exp(md[:, at] - lse))
            o = part if o is None else o + part
            first += nb * rows
        if r * 128 < half:
            keep_ref[at, :] = o
        else:
            send_ref[r * 128 - half : (r + 1) * 128 - half, :] = o
    loss = jnp.sum(lse_ref[:, :rows], axis=1, keepdims=True) - pos_ref[...]
    for ref in (keep_ref, send_ref):
        ref[half : half + 8, :] = jnp.broadcast_to(loss, (8, ref.shape[1]))


def sums(ps, mds, blocks, groups, lse, pos):
    rows, wide = blocks[0].shape[0] - META, blocks[0].shape[1]
    out = [jax.ShapeDtypeStruct((2 * rows + 8, wide), f32)] * 2
    return call(
        functools.partial(sums_kernel, groups, rows),
        out,
        *ps,
        *mds,
        *blocks,
        lse,
        pos,
        flops=2 * 4 * rows * len(blocks) * rows * wide,
        scratch=[pltpu.VMEM((len(blocks) * rows, wide), bf16)],
        limit=BIG,
    )


def log_add(a, b):
    top = jnp.maximum(a, b)
    return top + jnp.log(jnp.exp(a - top) + jnp.exp(b - top))


def tower_kernel(core_ref, own_ref, up_ref, dn_ref, qt_ref, feats_ref, tq_ref, keep_ref, give_ref):
    total = own_ref[...] + up_ref[...].astype(f32) + dn_ref[...].astype(f32)
    grad = ((total - qt_ref[...].astype(f32)) * 0.0625).astype(bf16)
    tower = dot(grad, feats_ref[...], 1, 0)
    first = core_ref[0] == 0

    def put(ref, v):
        for r in range(v.shape[0] // 128):
            for l in range(v.shape[1] // 128):
                ref[r * (v.shape[1] // 128) + l, :, :] = v[r * 128 : (r + 1) * 128, l * 128 : (l + 1) * 128]

    @pl.when(first)
    def _():
        put(keep_ref, tq_ref[...])
        put(give_ref, tower)

    @pl.when(jnp.logical_not(first))
    def _():
        put(keep_ref, tower)
        put(give_ref, tq_ref[...])


def finish_kernel(turn, core_ref, src_ref, *refs):
    gq_ref, gi_ref, out, sem = refs[-4:]
    across_tiles = out.shape[0] // 128
    for k in range(src_ref.shape[0]):
        r, l = divmod(k, across_tiles)
        out[l * 128 : (l + 1) * 128, r * 128 : (r + 1) * 128] = jnp.transpose(src_ref[k, :, :].astype(f32))

    @pl.when(core_ref[0] == turn)
    def _():
        copy = pltpu.make_async_copy(out, gq_ref, sem)
        copy.start()
        copy.wait()

    @pl.when(core_ref[0] != turn)
    def _():
        copy = pltpu.make_async_copy(out, gi_ref, sem)
        copy.start()
        copy.wait()


def finish(turn, core, src, shape, grads=()):
    any_spec = pl.BlockSpec(memory_space=pltpu.HBM)
    return pl.pallas_call(
        functools.partial(finish_kernel, turn),
        out_shape=[jax.ShapeDtypeStruct(shape, f32)] * 2,
        in_specs=[pl.BlockSpec(memory_space=pltpu.SMEM), pl.BlockSpec(memory_space=pltpu.VMEM)] + [any_spec] * len(grads),
        out_specs=[any_spec] * 2,
        scratch_shapes=[pltpu.VMEM(shape, f32), pltpu.SemaphoreType.DMA],
        input_output_aliases={2 + k: k for k in range(len(grads))},
        compiler_params=pltpu.CompilerParams(vmem_limit_bytes=LIMIT),
        name="finish",
    )(core, src, *grads)


def train_step(query_feats, item_feats, item_ids, bucket_ids, bucket_logq, query_tower, item_tower):
    query_input, item_input = query_feats[0], item_feats[0]
    rows, feats = query_input.shape
    wide = query_tower.shape[1]
    scaling = 1.0 / 16.0
    whole = pl.BlockSpec(memory_space=pltpu.VMEM)
    smem = pl.BlockSpec(memory_space=pltpu.SMEM)
    core = lax.axis_index("c").reshape(1)
    block = jax.ShapeDtypeStruct((rows + META, wide), bf16)
    sources = (item_ids, bucket_ids, bucket_logq.reshape(1, -1), item_input, item_tower, query_input, query_tower)
    query_block, item_block, positive = call(
        embed_kernel, (block, block, jax.ShapeDtypeStruct((1, 1), f32)), core, *sources,
        flops=4 * rows * feats * wide, specs=[smem] + [pl.BlockSpec(memory_space=pl.ANY)] * 7, limit=HUGE,
        scratch=[pltpu.VMEM((META, wide), f32), pltpu.SemaphoreType.DMA((7,))]
        + [pltpu.VMEM(a.shape, a.dtype) for a in sources],
    )

    up, dn = [item_block], [item_block]

    def ring(*after):
        u, d, _ = lax.optimization_barrier((up[-1], dn[-1], after))
        k = len(up)
        up.append(shift(u, "z", 1))
        if k < 4:
            dn.append(shift(d, "z", -1))

    ring()
    near = shift(query_block, "yh", 1)
    ring()
    query_near, item_near = call(fetch_kernel, (block, block), query_block, item_block)
    pair = jnp.concatenate([query_near, near])
    other = shift(pair, "c", 1)
    q, qt, ids = prep(pair, other)
    ring(ids)
    ps, mds, lse = [], [], None
    for k in range(5):
        p, md, lse = step(q, ids, [item_near] if k == 0 else [up[k]] if k == 4 else [up[k], dn[k]], lse)
        ps.append(p)
        mds.append(md)
        if k == 1:
            ring(lse)
    groups = [[item_near]] + [[up[k], dn[k]] for k in (1, 2, 3)] + [[up[4]]]

    row = jax.ShapeDtypeStruct(lse.shape, f32)
    lse = call(functools.partial(lse_kernel, 2, rows), row, lse, shift(lse, "c", 1))
    lse = call(functools.partial(lse_kernel, 1, rows), row, lse, shift(lse, "yh", 1))

    ring_up = shift(back(qt, ps[4], mds[4], lse, bf16)[0], "z", 1)
    ring_dn = None
    for k in (3, 2, 1):
        t_dn, t_up = back(qt, ps[k], mds[k], lse, bf16 if k == 3 else f32, f32)
        ring_up = shift((ring_up.astype(f32) + t_up).astype(bf16), "z", 1)
        ring_dn = t_dn if k == 3 else (ring_dn.astype(f32) + t_dn).astype(bf16)
        ring_dn = shift(ring_dn, "z", -1)
    t_own = back(qt, ps[0], mds[0], lse, f32)[0]
    flat = [b for blocks in groups for b in blocks]
    o_keep, o_send = sums(ps, mds, flat, [len(b) for b in groups], lse, positive)
    o_2 = o_keep + shift(o_send, "c", 1)
    o_y = shift(o_2[rows : 2 * rows].astype(bf16), "yh", 1)
    o = o_2[:rows] + o_y.astype(f32)
    query_grad = ((o - item_near[:rows].astype(f32)) * scaling).astype(bf16)
    tower_query = dot(query_grad, query_input, 0, 0)

    tiles = (wide // 128) * (feats // 128)
    out = [jax.ShapeDtypeStruct((tiles, 128, 128), f32)] * 2
    keep, give = call(
        tower_kernel, out, core, t_own, ring_up, ring_dn, qt[:, :rows], item_input, tower_query,
        flops=2 * rows * wide * feats, specs=[smem] + [whole] * 6,
    )
    plane = ("yh", "x", "yl")
    n, nz = lax.axis_size(plane), lax.axis_size("z")
    count = lax.axis_size(BLK) * rows * lax.axis_size(DP)
    sent = jax.ShapeDtypeStruct((n, 136, 128), bf16)
    sent = call(pack_kernel, sent, keep, shift(give, "c", 1), o_2[2 * rows :])
    got = lax.all_to_all(sent, plane, 0, 0, tiled=True)
    sent = call(plane_kernel, jax.ShapeDtypeStruct((nz, 136, 128), bf16), got)
    got = lax.all_to_all(sent, "z", 0, 0, tiled=True)
    out = (jax.ShapeDtypeStruct((n, 128, 128), bf16), jax.ShapeDtypeStruct((1, 128), f32))
    mine, loss = call(functools.partial(z_kernel, count), out, got)
    mine = lax.all_to_all(mine, plane, 0, 0, tiled=True)
    rest = shift(mine, "c", 1)
    grads = finish(0, core, mine, (feats, wide))
    grad_query, grad_item = finish(1, core, rest, (feats, wide), grads)
    return (grad_query, grad_item, loss[0, 0])


def solution(mesh):
    fine = Mesh(mesh.devices.reshape(2, 8, 2, 4, 2), ("yh", "z", "c", "x", "yl"))
    return jax.shard_map(
        train_step,
        mesh=fine,
        in_specs=(
            P(DP, BLK, None),
            P(DP, BLK, None),
            P(DP, BLK),
            P(DP, BLK),
            P(),
            P(),
            P(),
        ),
        out_specs=(P(), P(), P()),
        check_vma=False,
    )
```

```python
import functools

import jax
import jax.numpy as jnp
from jax import lax
from jax.experimental import pallas as pl
from jax.experimental.pallas import tpu as pltpu
from jax.sharding import Mesh
from jax.sharding import PartitionSpec as P

EXCLUDED = -1e30
BLK = ("yh", "z", "c")
DP = ("x", "yl")
META = 16
LIMIT, BIG, HUGE = 6 << 20, 8 << 20, 60 << 20

f32, bf16 = jnp.float32, jnp.bfloat16


def dot(a, b, ca, cb):
    return lax.dot_general(a, b, (((ca,), (cb,)), ((), ())), preferred_element_type=f32)


def shift(x, axis, by):
    n = lax.axis_size(axis)
    return lax.ppermute(x, axis, [(i, (i + by) % n) for i in range(n)])


def split3(x):
    hi = x.astype(bf16).astype(f32)
    mid = (x - hi).astype(bf16).astype(f32)
    return hi, mid, x - hi - mid


def join_meta(meta, at, scales):
    v = meta.astype(f32)
    left = sum(v[at + 2 * k : at + 2 * k + 1, :] * s for k, s in enumerate(scales))
    right = sum(v[at + 2 * k + 1 : at + 2 * k + 2, :128] * s for k, s in enumerate(scales))
    return jnp.concatenate([left, right], axis=1)


def ids_of(meta):
    return join_meta(meta, 0, (65536.0, 256.0, 1.0))


def corrections_of(meta):
    return join_meta(meta, 6, (1.0, 1.0, 1.0))


def eye():
    return lax.broadcasted_iota(jnp.int32, (128, 128), 0) == lax.broadcasted_iota(jnp.int32, (128, 128), 1)


def down(row):
    return jnp.sum(jnp.where(eye(), row, 0.0), axis=1, keepdims=True)


def across(col):
    return jnp.sum(jnp.where(eye(), col, 0.0), axis=0, keepdims=True)


def call(kernel, out_shape, *args, flops=0, scratch=(), limit=LIMIT, specs=None):
    size = sum(a.size * a.dtype.itemsize for a in args)
    extra = {} if specs is None else {"in_specs": specs}
    return pl.pallas_call(
        kernel,
        out_shape=out_shape,
        scratch_shapes=scratch,
        compiler_params=pltpu.CompilerParams(vmem_limit_bytes=limit),
        cost_estimate=pl.CostEstimate(flops=max(flops, 1), bytes_accessed=size, transcendentals=0),
        **extra,
    )(*args)


def embed_kernel(core_ref, *refs):
    sources, refs = refs[:7], refs[7:]
    q_out, i_out, pos_ref, *scratch = refs
    meta, sems, buffers = scratch[0], scratch[1], scratch[2:]
    copies = [pltpu.make_async_copy(s, d, sems.at[k]) for k, (s, d) in enumerate(zip(sources, buffers))]
    for c in copies:
        c.start()
    ids_ref, buckets_ref, logq_ref, item_ref, item_tower, query_ref, query_tower = buffers
    rows = item_ref.shape[0]
    for c in copies[:3]:
        c.wait()
    logq = logq_ref[...]
    nb = logq.shape[1]
    table = jnp.concatenate([down(logq[:, k : k + 128]) for k in range(0, nb, 128)], axis=0)
    hit = lax.broadcasted_iota(jnp.int32, (nb, rows), 0) == buckets_ref[...]
    correction = jnp.sum(jnp.where(hit, table, 0.0), axis=0, keepdims=True)
    ids = ids_ref[...]
    parts = [(ids >> 16).astype(f32), ((ids >> 8) & 255).astype(f32), (ids & 255).astype(f32)]
    meta[...] = jnp.zeros_like(meta)
    for k, v in enumerate((*parts, *split3(correction))):
        meta[2 * k : 2 * k + 1, :] = v[:, :256]
        meta[2 * k + 1 : 2 * k + 2, : rows - 256] = v[:, 256:]
    low = meta[...].astype(bf16)
    i_out[rows:, :] = low
    q_out[rows:, :] = low
    for c in copies[3:5]:
        c.wait()
    i_out[:rows, :] = dot(item_ref[...], item_tower[...], 1, 0).astype(bf16)
    for c in copies[5:]:
        c.wait()
    vecs = dot(query_ref[...], query_tower[...], 1, 0).astype(bf16)
    q_out[:rows, :] = vecs
    product = vecs.astype(f32) * i_out[:rows, :].astype(f32) * 0.0625
    total = jnp.sum(jnp.sum(product, axis=0, keepdims=True), axis=1, keepdims=True)
    pos_ref[...] = total - jnp.sum(correction, axis=1, keepdims=True)


def lse_kernel(bit, rows, mine_ref, other_ref, out_ref):
    for k in range(4):
        at, of = slice(k * rows, (k + 1) * rows), slice((k ^ bit) * rows, ((k ^ bit) + 1) * rows)
        out_ref[:, at] = log_add(mine_ref[:, at], other_ref[:, of])


def loss_rows(loss):
    row = lax.broadcasted_iota(jnp.int32, (8, 128), 0)
    hi, mid, lo = split3(loss)
    return jnp.where(row == 0, hi, jnp.where(row == 1, mid, jnp.where(row == 2, lo, 0.0)))


def pack_kernel(keep_ref, other_ref, loss_ref, out_ref):
    low = loss_rows(loss_ref[:1, :128]).astype(bf16)
    for k in range(keep_ref.shape[0]):
        out_ref[k, :128, :] = (keep_ref[k, :, :] + other_ref[k, :, :]).astype(bf16)
        out_ref[k, 128:, :] = low


def plane_kernel(in_ref, out_ref):
    total = sum(in_ref[k, :, :].astype(f32) for k in range(in_ref.shape[0]))
    low = loss_rows(jnp.sum(total[128:, :], axis=0, keepdims=True)).astype(bf16)
    top = total[:128, :].astype(bf16)
    for k in range(out_ref.shape[0]):
        out_ref[k, :128, :] = top
        out_ref[k, 128:, :] = low


def z_kernel(count, in_ref, out_ref, loss_ref):
    total = sum(in_ref[k, :, :].astype(f32) for k in range(in_ref.shape[0]))
    top = total[:128, :].astype(bf16)
    for k in range(out_ref.shape[0]):
        out_ref[k, :, :] = top
    loss_ref[...] = jnp.sum(total[128:, :], axis=0, keepdims=True) * (1.0 / count)


def prep_kernel(rows, b0, b2, q_ref, qt_ref, id_ref):
    full = rows + META
    for k, (b, at) in enumerate(((b0, 0), (b0, full), (b2, 0), (b2, full))):
        v = b[at : at + rows, :].astype(f32)
        q_ref[k * rows : (k + 1) * rows, :] = (v * 0.0625).astype(bf16)
        qt_ref[:, k * rows : (k + 1) * rows] = jnp.transpose(v).astype(bf16)
        ids = ids_of(b[at + rows : at + full, :])
        for j in range(rows // 128):
            id_ref[k * rows + j * 128 : k * rows + (j + 1) * 128, :] = jnp.broadcast_to(
                down(ids[:, j * 128 : (j + 1) * 128]), (128, 128)
            )


def prep(pair, other):
    rows, wide = pair.shape[0] // 2 - META, pair.shape[1]
    out = (
        jax.ShapeDtypeStruct((4 * rows, wide), bf16),
        jax.ShapeDtypeStruct((wide, 4 * rows), bf16),
        jax.ShapeDtypeStruct((4 * rows, 128), f32),
    )
    return call(functools.partial(prep_kernel, rows), out, pair, other, flops=10**8)


def step_kernel(first, nb, rows, tm, *refs):
    q_ref, id_ref = refs[:2]
    blocks = refs[2 : 2 + nb]
    at = 2 + nb
    if not first:
        lse_in = refs[at]
        at += 1
    p_ref, md_ref, lse_ref, items = refs[at:]
    for k, b in enumerate(blocks):
        items[k * rows : (k + 1) * rows, :] = b[:rows, :]
    metas = [b[rows : rows + META, :] for b in blocks]
    col_ids = jnp.concatenate([ids_of(m) for m in metas], axis=1)
    corr = jnp.concatenate([corrections_of(m) for m in metas], axis=1)
    cols = nb * rows

    def tile(t, carry):
        at = pl.ds(pl.multiple_of(t * tm, tm), tm)
        s = dot(q_ref[at, :], items[...], 1, 1) - corr
        dup = jnp.concatenate([id_ref[at, :]] * (cols // 128), axis=1) == col_ids
        if first:
            row = lax.broadcasted_iota(jnp.int32, (tm, cols), 0) + t * tm
            dup = dup & (row != lax.broadcasted_iota(jnp.int32, (tm, cols), 1))
        s = jnp.where(dup, EXCLUDED, s)
        m = jnp.max(s, axis=1, keepdims=True)
        p = jnp.exp(s - m)
        part = m + jnp.log(jnp.sum(p, axis=1, keepdims=True))
        p_ref[at, :] = p.astype(bf16)
        for j in range(tm // 128):
            sub = slice(j * 128, (j + 1) * 128)
            lane = pl.ds(pl.multiple_of(t * tm + j * 128, 128), 128)
            md_ref[:, lane] = across(m[sub])
            lse = across(part[sub])
            lse_ref[:, lane] = lse if first else log_add(lse_in[:, lane], lse)
        return carry

    lax.fori_loop(0, q_ref.shape[0] // tm, tile, 0, unroll=3)


def step(q, ids, blocks, lse, tm=256):
    n, wide = q.shape
    nb, rows = len(blocks), blocks[0].shape[0] - META
    row = jax.ShapeDtypeStruct((1, n), f32)
    return call(
        functools.partial(step_kernel, lse is None, nb, rows, tm),
        (jax.ShapeDtypeStruct((n, nb * rows), bf16), row, row),
        q,
        ids,
        *blocks,
        *(() if lse is None else (lse,)),
        flops=4 * n * nb * rows * wide,
        scratch=[pltpu.VMEM((nb * rows, wide), bf16)],
    )


def back_kernel(qt_ref, p_ref, md_ref, lse_ref, *outs):
    w = jnp.exp(md_ref[...] - lse_ref[...])
    qw = (qt_ref[...].astype(f32) * w).astype(bf16)
    t = dot(qw, p_ref[...], 1, 0)
    rows = t.shape[1] // len(outs)
    for k, o in enumerate(outs):
        o[...] = t[:, k * rows : (k + 1) * rows].astype(o.dtype)


def back(qt, p, md, lse, *dtypes):
    wide, n = qt.shape
    rows = p.shape[1] // len(dtypes)
    out = [jax.ShapeDtypeStruct((wide, rows), dtype) for dtype in dtypes]
    return call(back_kernel, out, qt, p, md, lse, flops=4 * n * p.shape[1] * wide)


def sums_kernel(groups, rows, *refs):
    n_p, n_b = len(groups), sum(groups)
    ps, mds = refs[:n_p], refs[n_p : 2 * n_p]
    blocks = refs[2 * n_p : 2 * n_p + n_b]
    lse_ref, pos_ref, keep_ref, send_ref, items = refs[2 * n_p + n_b :]
    for k, b in enumerate(blocks):
        items[k * rows : (k + 1) * rows, :] = b[:rows, :]
    half = 2 * rows
    for r in range(2 * half // 128):
        at = slice(r * 128, (r + 1) * 128)
        lse = lse_ref[:, at]
        o, first = None, 0
        for p, md, nb in zip(ps, mds, groups):
            part = dot(p[at, :], items[first : first + nb * rows, :], 1, 0) * down(jnp.exp(md[:, at] - lse))
            o = part if o is None else o + part
            first += nb * rows
        if r * 128 < half:
            keep_ref[at, :] = o
        else:
            send_ref[r * 128 - half : (r + 1) * 128 - half, :] = o
    loss = jnp.sum(lse_ref[:, :rows], axis=1, keepdims=True) - pos_ref[...]
    for ref in (keep_ref, send_ref):
        ref[half : half + 8, :] = jnp.broadcast_to(loss, (8, ref.shape[1]))


def sums(ps, mds, blocks, groups, lse, pos):
    rows, wide = blocks[0].shape[0] - META, blocks[0].shape[1]
    out = [jax.ShapeDtypeStruct((2 * rows + 8, wide), f32)] * 2
    return call(
        functools.partial(sums_kernel, groups, rows),
        out,
        *ps,
        *mds,
        *blocks,
        lse,
        pos,
        flops=2 * 4 * rows * len(blocks) * rows * wide,
        scratch=[pltpu.VMEM((len(blocks) * rows, wide), bf16)],
        limit=BIG,
    )


def log_add(a, b):
    top = jnp.maximum(a, b)
    return top + jnp.log(jnp.exp(a - top) + jnp.exp(b - top))


def tower_kernel(core_ref, own_ref, up_ref, dn_ref, qt_ref, feats_ref, tq_ref, keep_ref, give_ref):
    total = own_ref[...] + up_ref[...].astype(f32) + dn_ref[...].astype(f32)
    grad = ((total - qt_ref[...].astype(f32)) * 0.0625).astype(bf16)
    tower = dot(grad, feats_ref[...], 1, 0)
    first = core_ref[0] == 0

    def put(ref, v):
        for r in range(v.shape[0] // 128):
            for l in range(v.shape[1] // 128):
                ref[r * (v.shape[1] // 128) + l, :, :] = v[r * 128 : (r + 1) * 128, l * 128 : (l + 1) * 128]

    @pl.when(first)
    def _():
        put(keep_ref, tq_ref[...])
        put(give_ref, tower)

    @pl.when(jnp.logical_not(first))
    def _():
        put(keep_ref, tower)
        put(give_ref, tq_ref[...])


def finish_kernel(turn, core_ref, src_ref, *refs):
    gq_ref, gi_ref, out, sem = refs[-4:]
    across_tiles = out.shape[0] // 128
    for k in range(src_ref.shape[0]):
        r, l = divmod(k, across_tiles)
        out[l * 128 : (l + 1) * 128, r * 128 : (r + 1) * 128] = jnp.transpose(src_ref[k, :, :].astype(f32))

    @pl.when(core_ref[0] == turn)
    def _():
        copy = pltpu.make_async_copy(out, gq_ref, sem)
        copy.start()
        copy.wait()

    @pl.when(core_ref[0] != turn)
    def _():
        copy = pltpu.make_async_copy(out, gi_ref, sem)
        copy.start()
        copy.wait()


def finish(turn, core, src, shape, grads=()):
    any_spec = pl.BlockSpec(memory_space=pltpu.HBM)
    return pl.pallas_call(
        functools.partial(finish_kernel, turn),
        out_shape=[jax.ShapeDtypeStruct(shape, f32)] * 2,
        in_specs=[pl.BlockSpec(memory_space=pltpu.SMEM), pl.BlockSpec(memory_space=pltpu.VMEM)] + [any_spec] * len(grads),
        out_specs=[any_spec] * 2,
        scratch_shapes=[pltpu.VMEM(shape, f32), pltpu.SemaphoreType.DMA],
        input_output_aliases={2 + k: k for k in range(len(grads))},
        compiler_params=pltpu.CompilerParams(vmem_limit_bytes=LIMIT),
        name="finish",
    )(core, src, *grads)


def train_step(query_feats, item_feats, item_ids, bucket_ids, bucket_logq, query_tower, item_tower):
    query_input, item_input = query_feats[0], item_feats[0]
    rows, feats = query_input.shape
    wide = query_tower.shape[1]
    scaling = 1.0 / 16.0
    whole = pl.BlockSpec(memory_space=pltpu.VMEM)
    smem = pl.BlockSpec(memory_space=pltpu.SMEM)
    core = lax.axis_index("c").reshape(1)
    block = jax.ShapeDtypeStruct((rows + META, wide), bf16)
    sources = (item_ids, bucket_ids, bucket_logq.reshape(1, -1), item_input, item_tower, query_input, query_tower)
    near_block = pltpu.VMEM(block.shape, bf16)
    query_block, item_block, positive = call(
        embed_kernel, (near_block, near_block, pltpu.VMEM((1, 1), f32)), core, *sources,
        flops=4 * rows * feats * wide, specs=[smem] + [pl.BlockSpec(memory_space=pl.ANY)] * 7, limit=HUGE,
        scratch=[pltpu.VMEM((META, wide), f32), pltpu.SemaphoreType.DMA((7,))]
        + [pltpu.VMEM(a.shape, a.dtype) for a in sources],
    )

    up, dn = [item_block], [item_block]

    def ring(*after):
        u, d, _ = lax.optimization_barrier((up[-1], dn[-1], after))
        k = len(up)
        up.append(shift(u, "z", 1))
        if k < 4:
            dn.append(shift(d, "z", -1))

    ring()
    near = shift(query_block, "yh", 1)
    ring()
    pair = jnp.concatenate([query_block, near])
    other = shift(pair, "c", 1)
    q, qt, ids = prep(pair, other)
    ring(ids)
    ps, mds, lse = [], [], None
    for k in range(5):
        p, md, lse = step(q, ids, [item_block] if k == 0 else [up[k]] if k == 4 else [up[k], dn[k]], lse)
        ps.append(p)
        mds.append(md)
        if k == 0:
            ring(lse)
    groups = [[item_block]] + [[up[k], dn[k]] for k in (1, 2, 3)] + [[up[4]]]

    row = jax.ShapeDtypeStruct(lse.shape, f32)
    lse = call(functools.partial(lse_kernel, 2, rows), row, lse, shift(lse, "c", 1))
    lse = call(functools.partial(lse_kernel, 1, rows), row, lse, shift(lse, "yh", 1))

    ring_up = shift(back(qt, ps[4], mds[4], lse, bf16)[0], "z", 1)
    ring_dn = None
    for k in (3, 2, 1):
        t_dn, t_up = back(qt, ps[k], mds[k], lse, bf16 if k == 3 else f32, f32)
        ring_up = shift((ring_up.astype(f32) + t_up).astype(bf16), "z", 1)
        ring_dn = t_dn if k == 3 else (ring_dn.astype(f32) + t_dn).astype(bf16)
        ring_dn = shift(ring_dn, "z", -1)
    t_own = back(qt, ps[0], mds[0], lse, f32)[0]
    flat = [b for blocks in groups for b in blocks]
    o_keep, o_send = sums(ps, mds, flat, [len(b) for b in groups], lse, positive)
    o_2 = o_keep + shift(o_send, "c", 1)
    o_y = shift(o_2[rows : 2 * rows].astype(bf16), "yh", 1)
    o = o_2[:rows] + o_y.astype(f32)
    query_grad = ((o - item_block[:rows].astype(f32)) * scaling).astype(bf16)
    tower_query = dot(query_grad, query_input, 0, 0)

    tiles = (wide // 128) * (feats // 128)
    out = [jax.ShapeDtypeStruct((tiles, 128, 128), f32)] * 2
    keep, give = call(
        tower_kernel, out, core, t_own, ring_up, ring_dn, qt[:, :rows], item_input, tower_query,
        flops=2 * rows * wide * feats, specs=[smem] + [whole] * 6,
    )
    plane = ("yh", "x", "yl")
    n, nz = lax.axis_size(plane), lax.axis_size("z")
    count = lax.axis_size(BLK) * rows * lax.axis_size(DP)
    sent = jax.ShapeDtypeStruct((n, 136, 128), bf16)
    sent = call(pack_kernel, sent, keep, shift(give, "c", 1), o_2[2 * rows :])
    got = lax.all_to_all(sent, plane, 0, 0, tiled=True)
    sent = call(plane_kernel, jax.ShapeDtypeStruct((nz, 136, 128), bf16), got)
    got = lax.all_to_all(sent, "z", 0, 0, tiled=True)
    out = (jax.ShapeDtypeStruct((n, 128, 128), bf16), pltpu.VMEM((1, 128), f32))
    mine, loss = call(functools.partial(z_kernel, count), out, got)
    mine = lax.all_to_all(mine, plane, 0, 0, tiled=True)
    rest = shift(mine, "c", 1)
    grads = finish(0, core, mine, (feats, wide))
    grad_query, grad_item = finish(1, core, rest, (feats, wide), grads)
    return (grad_query, grad_item, loss[0, 0])


def solution(mesh):
    fine = Mesh(mesh.devices.reshape(2, 8, 2, 4, 2), ("yh", "z", "c", "x", "yl"))
    return jax.shard_map(
        train_step,
        mesh=fine,
        in_specs=(
            P(DP, BLK, None),
            P(DP, BLK, None),
            P(DP, BLK),
            P(DP, BLK),
            P(),
            P(),
            P(),
        ),
        out_specs=(P(), P(), P()),
        check_vma=False,
    )
```
